256 devices in a mesh: gx: 32 (over x_hi, z, core), gy: 8 (over y, x_lo).
Axes of the slice: x: 4 (x_hi: 2, x_lo: 2; x = x_hi * 2 + x_lo), y: 4, z: 8, core: 2. Of those that a mesh axis runs over, the one named last changes fastest.
Arguments:
- density: float32 [64, 24, 27648], P('gx', None, 'gy'), may hold values from 0.05 to 1
- gains_a: float32 [8, 24, 24, 24], replicated, may hold values from -6 to 6
- gains_b: float32 [8, 24, 24, 24], replicated, may hold values from -6 to 6
- loss_rates: float32 [24, 24, 24], replicated, may hold values from 0.1 to 1
Outputs:
- evolved: float32 [64, 24, 27648], P('gx', None, 'gy')
The draws below stay inside these ranges and needn't reach their ends.
All inputs are finite; a program needn't handle non-finite values.
Results may differ from the reference program's by a relative error of at most 0.0001.
Values sent between devices are 32-bit elements; how exact they have to be, the bound alone decides.
A program may use at most 128 MiB of HBM per device.

```python
import math
import jax
import jax.numpy as jnp
from jax import lax

V = 24
P_SIZE = 8
NX = 64
NY = 48


def level_of(own_key, dims, split, least, top_value):
    def one(axis_at, parts):
        draws = jax.random.uniform(jax.random.fold_in(jax.random.fold_in(own_key, 6), axis_at), (parts,), jnp.float32, least / len(split), top_value / len(split))
        return jnp.repeat(jnp.exp(draws), dims[axis_at] // parts).reshape((-1,) + (1,) * (len(dims) - axis_at - 1))

    loudness = one(*split[0])
    for cut in split[1:]:
        loudness = loudness * one(*cut)
    return loudness


def scatter_about(rng, dims, spread, most, held_as=jnp.bfloat16):
    return jnp.clip(spread * jax.random.normal(rng, dims, jnp.float32), -most, most).astype(held_as)


def setup_inputs(seed: int = 0) -> dict:
    splits = jax.random.split(jax.random.key(seed), 5)
    return {
        "density": jnp.clip(jnp.exp(math.log(1.0) - 2.9957323 * jax.random.uniform(splits[0], (NX, V, NY * V * V), jnp.float32) ** level_of(splits[0], (NX, V, NY * V * V), ((0, 32), (2, 8)), -0.2, 0.2)), 0.05, 1.0),
        "gains_a": scatter_about(splits[1], (P_SIZE, V, V, V), 1.0, 6.0, jnp.float32),
        "gains_b": scatter_about(splits[2], (P_SIZE, V, V, V), 1.0, 6.0, jnp.float32),
        "loss_rates": jnp.clip(jnp.exp(jax.random.uniform(splits[3], (V, V, V), jnp.float32, math.log(0.1), math.log(1.0))), 0.1, 1.0),
    }


highest = lax.Precision.HIGHEST
courant_max = 1.6
collide_step = 0.2

def cosine_table(count):
    freq = jnp.arange(count, dtype=jnp.float32)[:, None]
    points = jnp.arange(count, dtype=jnp.float32)[None, :]
    scale = jnp.where(freq == 0, jnp.sqrt(1.0 / count), jnp.sqrt(2.0 / count))
    return scale * jnp.cos(jnp.pi * (2.0 * points + 1.0) * freq / (2.0 * count))

def courant(count):
    speeds = jnp.arange(count, dtype=jnp.float32) - (count - 1) / 2.0
    return courant_max * jnp.abs(speeds) / ((count - 1) / 2.0)

def weights(numbers):
    return (1.0 - 1.5 * numbers + 0.5 * numbers * numbers, 2.0 * numbers - numbers * numbers, 0.5 * (numbers * numbers - numbers))

def transform(table, field):
    field = jnp.einsum('ka,xaybc->xkybc', table, field, precision=highest)
    field = jnp.einsum('kb,xaybc->xaykc', table, field, precision=highest)
    return jnp.einsum('kc,xaybc->xaybk', table, field, precision=highest)

def collide(field, cosine, gains_a, gains_b, loss_rates):
    spectrum = transform(cosine, field)
    loss = field * transform(cosine.T, loss_rates[:, None, :, :] * spectrum)
    gain = jnp.zeros_like(field)
    for term in range(gains_a.shape[0]):
        first = transform(cosine.T, gains_a[term][:, None, :, :] * spectrum)
        second = transform(cosine.T, gains_b[term][:, None, :, :] * spectrum)
        gain = gain + first * second
    return field + collide_step * (gain - loss)

def reference(density, gains_a, gains_b, loss_rates):
    middle = V // 2
    numbers = courant(V)
    cosine = cosine_table(V)
    field = density.reshape(NX, V, NY, V, V)
    pw0, pw1, pw2 = weights(numbers[middle:][None, :, None, None, None])
    nw0, nw1, nw2 = weights(numbers[:middle][None, :, None, None, None])
    positive = field[:, middle:]
    negative = field[:, :middle]
    pos_new = pw0 * positive + pw1 * jnp.roll(positive, 1, 0) + pw2 * jnp.roll(positive, 2, 0)
    neg_new = nw0 * negative + nw1 * jnp.roll(negative, -1, 0) + nw2 * jnp.roll(negative, -2, 0)
    field = jnp.concatenate([neg_new, pos_new], 1)
    field = collide(field, cosine, gains_a, gains_b, loss_rates)
    pw0, pw1, pw2 = weights(numbers[middle:][None, None, None, :, None])
    nw0, nw1, nw2 = weights(numbers[:middle][None, None, None, :, None])
    positive = field[:, :, :, middle:]
    negative = field[:, :, :, :middle]
    pos_new = pw0 * positive + pw1 * jnp.roll(positive, 1, 2) + pw2 * jnp.roll(positive, 2, 2)
    neg_new = nw0 * negative + nw1 * jnp.roll(negative, -1, 2) + nw2 * jnp.roll(negative, -2, 2)
    field = jnp.concatenate([neg_new, pos_new], 3)
    field = collide(field, cosine, gains_a, gains_b, loss_rates)
    return field.reshape(NX, V, NY * V * V)
```

```python
import functools

import jax
import jax.numpy as jnp
import numpy as np
from jax import lax
from jax.experimental import pallas as pl
from jax.experimental.pallas import tpu as pltpu
from jax.sharding import PartitionSpec as P

COUNT = 24
HALF = COUNT // 2
PLACES = HALF * HALF
LANES = 128
CELLS = 4
CHUNK = 16
collide_step = 0.2
courant_max = 1.6
f32 = jnp.float32


def cosine_table():
    freq = np.arange(COUNT)[:, None]
    points = np.arange(COUNT)[None, :]
    scale = np.where(freq == 0, np.sqrt(1.0 / COUNT), np.sqrt(2.0 / COUNT))
    return scale * np.cos(np.pi * (2 * points + 1) * freq / (2 * COUNT))


def two_parts(table):
    high = table.astype(jnp.bfloat16)
    return high, (table - high.astype(np.float64)).astype(jnp.bfloat16)


def transform_tables():
    cosine = cosine_table()
    plane = []
    for parity_x in range(2):
        for parity_y in range(2):
            along_x, along_y = cosine[parity_x::2, :HALF], cosine[parity_y::2, :HALF]
            plane.append(np.einsum("jn,lm->mnjl", along_x, along_y).reshape(PLACES, PLACES))
    plane = np.stack(plane)

    def stacked(table):
        return np.concatenate(two_parts(table), 1)

    def line(table):
        used = CELLS * COUNT
        wide = np.zeros((LANES, LANES))
        wide[:used, :used] = np.kron(np.eye(CELLS), table)
        high, low = two_parts(wide)
        return np.block([[high, low], [high, np.zeros_like(high)]])

    return stacked(plane.transpose(0, 2, 1)), line(cosine.T), stacked(plane), line(cosine)


def weights():
    speeds = np.arange(COUNT) - (COUNT - 1) / 2
    numbers = courant_max * np.abs(speeds) / ((COUNT - 1) / 2)
    return np.stack([1 - 1.5 * numbers + 0.5 * numbers**2, 2 * numbers - numbers**2, 0.5 * (numbers**2 - numbers)])


def x_weights():
    return np.broadcast_to(weights().reshape(3, 2, HALF, 1), (3, 2, HALF, LANES)).astype(np.float32)


def y_weights():
    both = weights().reshape(3, 2, HALF)
    both = np.stack([both[:, 0], both[:, 1, ::-1]], 1)
    both = np.repeat(both, HALF, 2)[..., None]
    return np.broadcast_to(both, (3, 2, PLACES, LANES)).astype(np.float32)


def split(value):
    high = value.astype(jnp.bfloat16)
    return high, (value - high.astype(f32)).astype(jnp.bfloat16)


def line_transform(value, table):
    both = jnp.dot(jnp.concatenate(split(value), 1), table, preferred_element_type=f32)
    return both[:, :LANES] + both[:, LANES:]


def plane_transform(value, table):
    high, low = split(value)
    first = jnp.dot(table, high, preferred_element_type=f32)
    second = jnp.dot(table[:PLACES], low, preferred_element_type=f32)
    return first[:PLACES] + first[PLACES:] + second


def butterfly(parts):
    sum_0, diff_0 = parts[0] + parts[1], parts[0] - parts[1]
    sum_1, diff_1 = parts[2] + parts[3], parts[2] - parts[3]
    return sum_0 + sum_1, diff_0 + diff_1, sum_0 - sum_1, diff_0 - diff_1


def block(index):
    return slice(index * LANES, (index + 1) * LANES)


def side_by_side(value, parts):
    return jnp.concatenate([value[i * PLACES : (i + 1) * PLACES] for i in range(parts)], 1)


def backward(groups, factors, modes, mixed, plane, line):
    for q in range(4):
        scaled = [modes[q, :, block(g)] * factor(q) for factor in factors for g in range(groups)]
        moved = line_transform(jnp.concatenate(scaled, 0), line[...])
        mixed[q, :, : len(scaled) * LANES] = plane_transform(side_by_side(moved, len(scaled)), plane[q])


def forward(groups, field, modes, mixed, plane, line):
    wide = groups * LANES
    for start in range(0, PLACES, CHUNK):
        rows = slice(start, start + CHUNK)
        parts = butterfly([field[q, rows, :] for q in range(4)])
        for q in range(4):
            mixed[q, rows, :wide] = parts[q]
    for q in range(4):
        moved = plane_transform(mixed[q, :, :wide], plane[q])
        stacked = jnp.concatenate([moved[:, block(g)] for g in range(groups)], 0)
        modes[q] = side_by_side(line_transform(stacked, line[...]), groups)


def collide_term(groups, field, total, modes, mixed, gain_a, gain_b, loss, tables):
    plane_fwd, line_fwd, plane_back, line_back = tables
    wide = groups * LANES

    @pl.when(pl.program_id(0) == 0)
    def _():
        forward(groups, field, modes, mixed, plane_fwd, line_fwd)
        backward(groups, [lambda q: loss[q]], modes, mixed, plane_back, line_back)
        for start in range(0, PLACES, CHUNK):
            rows = slice(start, start + CHUNK)
            parts = butterfly([mixed[q, rows, :wide] for q in range(4)])
            for q in range(4):
                total[q, rows, :] = -field[q, rows, :] * parts[q]

    backward(groups, [lambda q: gain_a[0, q], lambda q: gain_b[0, q]], modes, mixed, plane_back, line_back)
    for start in range(0, PLACES, CHUNK):
        rows = slice(start, start + CHUNK)
        first = butterfly([mixed[q, rows, :wide] for q in range(4)])
        second = butterfly([mixed[q, rows, wide : 2 * wide] for q in range(4)])
        for q in range(4):
            total[q, rows, :] += first[q] * second[q]


def piece(y, cell_x, cell_y):
    return cell_y * COUNT * COUNT + y * COUNT


def x_kernel(groups, density, below, above, weight, gain_a, gain_b, loss, *refs):
    tables, (out, lower, upper, swept, field, total, modes, mixed) = refs[:4], refs[4:]

    @pl.when(pl.program_id(0) == 0)
    def _():
        neg = [density[c, :HALF, :] for c in range(2)] + [above[:HALF, :], above[HALF:, :]]
        nw = [weight[k, 0, :, :1] for k in range(3)]
        for c in range(2):
            swept[c, 0, :HALF, :] = nw[0] * neg[c] + nw[1] * neg[c + 1] + nw[2] * neg[c + 2]
        pos = [below[:HALF, :], below[HALF:, :]] + [density[c, HALF:, :] for c in range(2)]
        pw = [weight[k, 1, :, :1] for k in range(3)]
        for c in range(2):
            new = pw[0] * pos[c + 2] + pw[1] * pos[c + 1] + pw[2] * pos[c]
            for row in range(HALF):
                swept[c, 1, HALF - 1 - row : HALF - row, :] = new[row : row + 1]
        for half_y in range(2):
            for place in range(HALF):
                y = COUNT - 1 - place if half_y else place
                for half_x in range(2):
                    for g in range(groups):
                        parts = []
                        for s in range(CELLS):
                            at = piece(y, s // 2, 2 * g + s % 2)
                            parts.append(swept[s // 2, half_x, :HALF, at : at + COUNT])
                        parts.append(jnp.zeros((HALF, LANES - CELLS * COUNT), f32))
                        field[2 * half_x + half_y, place * HALF : (place + 1) * HALF, block(g)] = jnp.concatenate(parts, 1)

    collide_term(groups, field, total, modes, mixed, gain_a, gain_b, loss, tables)

    @pl.when(pl.program_id(0) == pl.num_programs(0) - 1)
    def _():
        for q in range(4):
            out[q] = field[q] + collide_step * total[q]
        for half_x in range(2):
            lower[half_x] = out[2 * half_x, :, block(0)]
            upper[half_x] = out[2 * half_x + 1, :, block(groups - 1)]


def y_kernel(groups, before, below, above, weight, gain_a, gain_b, loss, *refs):
    tables, (out, swept, field, total, modes, mixed) = refs[:4], refs[4:]

    @pl.when(pl.program_id(0) == 0)
    def _():
        place = lax.broadcasted_iota(jnp.int32, (PLACES, LANES), 1) // COUNT
        odd = place % 2 == 1
        for half_x in range(2):
            for half_y in range(2):
                q = 2 * half_x + half_y
                w0, w1, w2 = [weight[k, half_y] for k in range(3)]
                blocks = [before[q, :, block(g)] for g in range(groups)]
                blocks = [below[half_x]] + blocks if half_y else blocks + [above[half_x]]
                right = [pltpu.roll(b, COUNT, 1) for b in blocks]
                left = [pltpu.roll(b, LANES - COUNT, 1) for b in blocks]
                for g in range(groups):
                    if half_y:
                        near = jnp.where(odd, right[g + 1], left[g])
                        new = w0 * blocks[g + 1] + w1 * near + w2 * blocks[g]
                    else:
                        near = jnp.where(odd, right[g + 1], left[g])
                        new = w0 * blocks[g] + w1 * near + w2 * blocks[g + 1]
                    field[q, :, block(g)] = new

    collide_term(groups, field, total, modes, mixed, gain_a, gain_b, loss, tables)

    @pl.when(pl.program_id(0) == pl.num_programs(0) - 1)
    def _():
        for q in range(4):
            field[q] = field[q] + collide_step * total[q]
        for half_x in range(2):
            for c in range(2):
                for g in range(groups):
                    parts = []
                    for cell_y in range(2):
                        for y in range(COUNT):
                            half_y, place = (0, y) if y < HALF else (1, COUNT - 1 - y)
                            at = g * LANES + (2 * c + cell_y) * COUNT
                            parts.append(field[2 * half_x + half_y, place * HALF : (place + 1) * HALF, at : at + COUNT])
                    wide = 2 * COUNT * COUNT
                    swept[c, half_x, :HALF, g * wide : (g + 1) * wide] = jnp.concatenate(parts, 1)
        for c in range(2):
            out[c, :HALF, :] = swept[c, 0, :HALF, :]
            for row in range(HALF):
                out[c, HALF + row : HALF + row + 1, :] = swept[c, 1, HALF - 1 - row : HALF - row, :]


def whole(array):
    return pl.BlockSpec(array.shape, lambda p: (0,) * array.ndim)


def call(kernel, groups, terms, field_args, gains, tables, out_shapes, scratch):
    gain = pl.BlockSpec((1, 4, PLACES, LANES), lambda p: (p, 0, 0, 0))
    wide = groups * LANES
    return pl.pallas_call(
        functools.partial(kernel, groups),
        grid=(terms,),
        out_shape=out_shapes,
        in_specs=[whole(a) for a in field_args] + [gain, gain, whole(gains[2])] + [whole(t) for t in tables],
        out_specs=jax.tree.map(whole, out_shapes),
        scratch_shapes=scratch
        + [pltpu.VMEM((4, PLACES, n * wide), f32) for n in (1, 1, 1, 2)],
    )(*field_args, *gains, *tables)


def by_parity(factor):
    terms = factor.shape[0]
    factor = factor.reshape(terms, HALF, 2, HALF, 2, COUNT).transpose(0, 2, 4, 1, 3, 5).reshape(terms, 4, PLACES, COUNT)
    return jnp.pad(jnp.concatenate([factor] * CELLS, -1), ((0, 0),) * 3 + ((0, LANES - CELLS * COUNT),))


def passed_along(value, axis, steps):
    count = lax.axis_size(axis)
    pairs = [(source, (source + steps) % count) for source in range(count)]
    return lax.ppermute(value, axis, pairs)


def body(density, gains_a, gains_b, loss_rates):
    cells_x, count, merged = density.shape
    terms = gains_a.shape[0]
    groups = merged // (2 * count * count)
    below = passed_along(density[:, HALF:].reshape(count, merged), "gx", 1)
    above = passed_along(density[:, :HALF].reshape(count, merged), "gx", -1)
    gains = (by_parity(gains_a), by_parity(gains_b), by_parity(loss_rates[None])[0])
    tables = tuple(jnp.asarray(t) for t in transform_tables())
    inner = jax.ShapeDtypeStruct((4, PLACES, groups * LANES), f32)
    rim = jax.ShapeDtypeStruct((2, PLACES, LANES), f32)
    swept = pltpu.VMEM((2, 2, 16, merged), f32)
    field, lower, upper = call(
        x_kernel, groups, terms, (density, below, above, jnp.asarray(x_weights())), gains, tables, (inner, rim, rim), [swept]
    )
    below = passed_along(upper, "gy", 1)
    above = passed_along(lower, "gy", -1)
    out = jax.ShapeDtypeStruct(density.shape, f32)
    return call(y_kernel, groups, terms, (field, below, above, jnp.asarray(y_weights())), gains, tables, out, [swept])


def solution(mesh):
    in_specs = (P("gx", None, "gy"), P(), P(), P())
    out_specs = P("gx", None, "gy")
    return jax.shard_map(body, mesh=mesh, in_specs=in_specs, out_specs=out_specs, check_vma=False)
```

```python
import functools

import jax
import jax.numpy as jnp
import numpy as np
from jax import lax
from jax.experimental import pallas as pl
from jax.experimental.pallas import tpu as pltpu
from jax.sharding import PartitionSpec as P

COUNT = 24
HALF = COUNT // 2
PLACES = HALF * HALF
LANES = 128
CELLS = 4
CHUNK = 16
collide_step = 0.2
courant_max = 1.6
f32 = jnp.float32


def cosine_table():
    freq = np.arange(COUNT)[:, None]
    points = np.arange(COUNT)[None, :]
    scale = np.where(freq == 0, np.sqrt(1.0 / COUNT), np.sqrt(2.0 / COUNT))
    return scale * np.cos(np.pi * (2 * points + 1) * freq / (2 * COUNT))


def two_parts(table):
    high = table.astype(jnp.bfloat16)
    return high, (table - high.astype(np.float64)).astype(jnp.bfloat16)


def transform_tables():
    cosine = cosine_table()
    plane = []
    for parity_x in range(2):
        for parity_y in range(2):
            along_x, along_y = cosine[parity_x::2, :HALF], cosine[parity_y::2, :HALF]
            plane.append(np.einsum("jn,lm->mnjl", along_x, along_y).reshape(PLACES, PLACES))
    plane = np.stack(plane)

    def stacked(table):
        return np.concatenate(two_parts(table), 1)

    def line(table):
        used = CELLS * COUNT
        wide = np.zeros((LANES, LANES))
        wide[:used, :used] = np.kron(np.eye(CELLS), table)
        high, low = two_parts(wide)
        return np.block([[high, low], [high, np.zeros_like(high)]])

    return stacked(plane.transpose(0, 2, 1)), line(cosine.T), stacked(plane), line(cosine)


def weights():
    speeds = np.arange(COUNT) - (COUNT - 1) / 2
    numbers = courant_max * np.abs(speeds) / ((COUNT - 1) / 2)
    return np.stack([1 - 1.5 * numbers + 0.5 * numbers**2, 2 * numbers - numbers**2, 0.5 * (numbers**2 - numbers)])


def x_weights():
    return np.broadcast_to(weights().reshape(3, 2, HALF, 1), (3, 2, HALF, LANES)).astype(np.float32)


def y_weights():
    both = weights().reshape(3, 2, HALF)
    both = np.stack([both[:, 0], both[:, 1, ::-1]], 1)
    both = np.repeat(both, HALF, 2)[..., None]
    return np.broadcast_to(both, (3, 2, PLACES, LANES)).astype(np.float32)


def split(value):
    high = value.astype(jnp.bfloat16)
    return high, (value - high.astype(f32)).astype(jnp.bfloat16)


def line_transform(value, table):
    both = jnp.dot(jnp.concatenate(split(value), 1), table, preferred_element_type=f32)
    return both[:, :LANES] + both[:, LANES:]


def plane_transform(value, table):
    high, low = split(value)
    first = jnp.dot(table, high, preferred_element_type=f32)
    second = jnp.dot(table[:PLACES], low, preferred_element_type=f32)
    return first[:PLACES] + first[PLACES:] + second


def butterfly(parts):
    sum_0, diff_0 = parts[0] + parts[1], parts[0] - parts[1]
    sum_1, diff_1 = parts[2] + parts[3], parts[2] - parts[3]
    return sum_0 + sum_1, diff_0 + diff_1, sum_0 - sum_1, diff_0 - diff_1


def block(index):
    return slice(index * LANES, (index + 1) * LANES)


def side_by_side(value, parts):
    return jnp.concatenate([value[i * PLACES : (i + 1) * PLACES] for i in range(parts)], 1)


def backward(groups, factors, modes, mixed, plane, line):
    parts = []
    for q in range(4):
        scaled = [modes[q, :, block(g)] * factor(q) for factor in factors for g in range(groups)]
        moved = plane_transform(jnp.concatenate(scaled, 1), plane[q])
        parts += [moved[:, block(i)] for i in range(len(scaled))]
    moved = line_transform(jnp.concatenate(parts, 0), line[...])
    count = len(factors) * groups
    for q in range(4):
        mixed[q, :, : count * LANES] = side_by_side(moved[q * count * PLACES : (q + 1) * count * PLACES], count)


def forward(groups, field, modes, mixed, plane, line):
    wide = groups * LANES
    for start in range(0, PLACES, CHUNK):
        rows = slice(start, start + CHUNK)
        parts = butterfly([field[q, rows, :] for q in range(4)])
        for q in range(4):
            mixed[q, rows, :wide] = parts[q]
    for q in range(4):
        moved = plane_transform(mixed[q, :, :wide], plane[q])
        stacked = jnp.concatenate([moved[:, block(g)] for g in range(groups)], 0)
        modes[q] = side_by_side(line_transform(stacked, line[...]), groups)


def collide_term(groups, field, total, modes, mixed, gain_a, gain_b, loss, tables):
    plane_fwd, line_fwd, plane_back, line_back = tables
    wide = groups * LANES

    @pl.when(pl.program_id(0) == 0)
    def _():
        forward(groups, field, modes, mixed, plane_fwd, line_fwd)
        backward(groups, [lambda q: loss[q]], modes, mixed, plane_back, line_back)
        for start in range(0, PLACES, CHUNK):
            rows = slice(start, start + CHUNK)
            parts = butterfly([mixed[q, rows, :wide] for q in range(4)])
            for q in range(4):
                total[q, rows, :] = -field[q, rows, :] * parts[q]

    backward(groups, [lambda q: gain_a[0, q], lambda q: gain_b[0, q]], modes, mixed, plane_back, line_back)
    for start in range(0, PLACES, CHUNK):
        rows = slice(start, start + CHUNK)
        first = butterfly([mixed[q, rows, :wide] for q in range(4)])
        second = butterfly([mixed[q, rows, wide : 2 * wide] for q in range(4)])
        for q in range(4):
            total[q, rows, :] += first[q] * second[q]


def piece(y, cell_x, cell_y):
    return cell_y * COUNT * COUNT + y * COUNT


def x_kernel(groups, density, below, above, weight, gain_a, gain_b, loss, *refs):
    tables, (out, lower, upper, swept, field, total, modes, mixed) = refs[:4], refs[4:]

    @pl.when(pl.program_id(0) == 0)
    def _():
        neg = [density[c, :HALF, :] for c in range(2)] + [above[:HALF, :], above[HALF:, :]]
        nw = [weight[k, 0, :, :1] for k in range(3)]
        for c in range(2):
            swept[c, 0, :HALF, :] = nw[0] * neg[c] + nw[1] * neg[c + 1] + nw[2] * neg[c + 2]
        pos = [below[:HALF, :], below[HALF:, :]] + [density[c, HALF:, :] for c in range(2)]
        pw = [weight[k, 1, :, :1] for k in range(3)]
        for c in range(2):
            new = pw[0] * pos[c + 2] + pw[1] * pos[c + 1] + pw[2] * pos[c]
            for row in range(HALF):
                swept[c, 1, HALF - 1 - row : HALF - row, :] = new[row : row + 1]
        for half_y in range(2):
            for place in range(HALF):
                y = COUNT - 1 - place if half_y else place
                for half_x in range(2):
                    for g in range(groups):
                        parts = []
                        for s in range(CELLS):
                            at = piece(y, s // 2, 2 * g + s % 2)
                            parts.append(swept[s // 2, half_x, :HALF, at : at + COUNT])
                        parts.append(jnp.zeros((HALF, LANES - CELLS * COUNT), f32))
                        field[2 * half_x + half_y, place * HALF : (place + 1) * HALF, block(g)] = jnp.concatenate(parts, 1)

    collide_term(groups, field, total, modes, mixed, gain_a, gain_b, loss, tables)

    @pl.when(pl.program_id(0) == pl.num_programs(0) - 1)
    def _():
        for q in range(4):
            out[q] = field[q] + collide_step * total[q]
        for half_x in range(2):
            lower[half_x] = out[2 * half_x, :, block(0)]
            upper[half_x] = out[2 * half_x + 1, :, block(groups - 1)]


def y_kernel(groups, before, below, above, weight, gain_a, gain_b, loss, *refs):
    tables, (out, swept, field, total, modes, mixed) = refs[:4], refs[4:]

    @pl.when(pl.program_id(0) == 0)
    def _():
        place = lax.broadcasted_iota(jnp.int32, (PLACES, LANES), 1) // COUNT
        odd = place % 2 == 1
        for half_x in range(2):
            for half_y in range(2):
                q = 2 * half_x + half_y
                w0, w1, w2 = [weight[k, half_y] for k in range(3)]
                blocks = [before[q, :, block(g)] for g in range(groups)]
                blocks = [below[half_x]] + blocks if half_y else blocks + [above[half_x]]
                right = [pltpu.roll(b, COUNT, 1) for b in blocks]
                left = [pltpu.roll(b, LANES - COUNT, 1) for b in blocks]
                for g in range(groups):
                    if half_y:
                        near = jnp.where(odd, right[g + 1], left[g])
                        new = w0 * blocks[g + 1] + w1 * near + w2 * blocks[g]
                    else:
                        near = jnp.where(odd, right[g + 1], left[g])
                        new = w0 * blocks[g] + w1 * near + w2 * blocks[g + 1]
                    field[q, :, block(g)] = new

    collide_term(groups, field, total, modes, mixed, gain_a, gain_b, loss, tables)

    @pl.when(pl.program_id(0) == pl.num_programs(0) - 1)
    def _():
        for q in range(4):
            field[q] = field[q] + collide_step * total[q]
        for half_x in range(2):
            for c in range(2):
                for g in range(groups):
                    parts = []
                    for cell_y in range(2):
                        for y in range(COUNT):
                            half_y, place = (0, y) if y < HALF else (1, COUNT - 1 - y)
                            at = g * LANES + (2 * c + cell_y) * COUNT
                            parts.append(field[2 * half_x + half_y, place * HALF : (place + 1) * HALF, at : at + COUNT])
                    wide = 2 * COUNT * COUNT
                    swept[c, half_x, :HALF, g * wide : (g + 1) * wide] = jnp.concatenate(parts, 1)
        for c in range(2):
            out[c, :HALF, :] = swept[c, 0, :HALF, :]
            for row in range(HALF):
                out[c, HALF + row : HALF + row + 1, :] = swept[c, 1, HALF - 1 - row : HALF - row, :]


def whole(array):
    return pl.BlockSpec(array.shape, lambda p: (0,) * array.ndim)


def call(kernel, groups, terms, field_args, gains, tables, out_shapes, scratch):
    gain = pl.BlockSpec((1, 4, PLACES, LANES), lambda p: (p, 0, 0, 0))
    wide = groups * LANES
    return pl.pallas_call(
        functools.partial(kernel, groups),
        grid=(terms,),
        out_shape=out_shapes,
        in_specs=[whole(a) for a in field_args] + [gain, gain, whole(gains[2])] + [whole(t) for t in tables],
        out_specs=jax.tree.map(whole, out_shapes),
        scratch_shapes=scratch
        + [pltpu.VMEM((4, PLACES, n * wide), f32) for n in (1, 1, 1, 2)],
    )(*field_args, *gains, *tables)


def meet(axis):
    count = lax.axis_size(axis)
    me = lax.axis_index(axis)
    after, before = {axis: lax.rem(me + 1, count)}, {axis: lax.rem(me + count - 1, count)}
    barrier = pltpu.get_barrier_semaphore()
    for neighbour in (after, before):
        pl.semaphore_signal(barrier, inc=1, device_id=neighbour, device_id_type=pl.DeviceIdType.MESH)
    return barrier, after, before


def passed(source, target, device, sends, receives, index):
    return pltpu.make_async_remote_copy(
        src_ref=source,
        dst_ref=target,
        send_sem=sends.at[index],
        recv_sem=receives.at[index],
        device_id=device,
        device_id_type=pl.DeviceIdType.MESH,
    )


def spread(raw, wide, out):
    used = lax.broadcasted_iota(jnp.int32, (COUNT, LANES), 1) < COUNT
    for mode in range(COUNT):
        value = jnp.concatenate([raw[mode], jnp.zeros((COUNT, LANES - COUNT), f32)], 1)
        value = jnp.where(used, value, 0.0)
        value = value + pltpu.roll(value, COUNT, 1)
        wide[mode] = value + pltpu.roll(value, 2 * COUNT, 1)
    for parity_x in range(2):
        for parity_y in range(2):
            rows = [wide[2 * place + parity_x, pl.ds(parity_y, HALF, stride=2), :] for place in range(HALF)]
            for place in range(0, HALF, 2):
                out[2 * parity_x + parity_y, place * HALF : (place + 2) * HALF, :] = jnp.concatenate(rows[place : place + 2], 0)


def start_kernel(density, gain_a, gain_b, loss, below, above, out_a, out_b, out_loss, *refs):
    up, down, raw_a, raw_b, raw_loss, wide, made_a, made_b, made_loss, sends, receives, loads, saves, load_loss, save_loss = refs
    terms = raw_a.shape[0]
    sides = ((0, gain_a, raw_a, made_a, out_a), (1, gain_b, raw_b, made_b, out_b))

    def load(p, side):
        i, source, raw, _, _ = sides[side]
        return pltpu.make_async_copy(source.at[p], raw.at[p], loads.at[i, p])

    def save(p, side):
        i, _, _, made, out = sides[side]
        return pltpu.make_async_copy(made.at[p], out.at[p], saves.at[i, p])

    pltpu.make_async_copy(loss, raw_loss, load_loss).start()
    for side in range(2):
        lax.fori_loop(0, terms, lambda p, c: (load(p, side).start(), c)[1], 0)
    barrier, after, before = meet("gx")
    for c in range(2):
        up[c * HALF : (c + 1) * HALF, :] = density[c, HALF:, :]
        down[c * HALF : (c + 1) * HALF, :] = density[c, :HALF, :]
    pl.semaphore_wait(barrier, 2)
    forth = passed(up, below, after, sends, receives, 0)
    back = passed(down, above, before, sends, receives, 1)
    forth.start()
    back.start()
    pltpu.make_async_copy(loss, raw_loss, load_loss).wait()
    spread(raw_loss, wide, made_loss)
    pltpu.make_async_copy(made_loss, out_loss, save_loss).start()
    for side in range(2):

        def one(p, carry):
            load(p, side).wait()
            spread(sides[side][2].at[p], wide, sides[side][3].at[p])
            save(p, side).start()
            return carry

        lax.fori_loop(0, terms, one, 0)
    for side in range(2):
        lax.fori_loop(0, terms, lambda p, c: (save(p, side).wait(), c)[1], 0)
    pltpu.make_async_copy(made_loss, out_loss, save_loss).wait()
    forth.wait()
    back.wait()


def start(density, gains_a, gains_b, loss_rates):
    terms = gains_a.shape[0]
    rim = jax.ShapeDtypeStruct((COUNT, density.shape[2]), f32)
    gain = jax.ShapeDtypeStruct((terms, 4, PLACES, LANES), f32)
    loss = jax.ShapeDtypeStruct((4, PLACES, LANES), f32)
    anywhere = pl.BlockSpec(memory_space=pl.ANY)
    dma = pltpu.SemaphoreType.DMA
    return pl.pallas_call(
        start_kernel,
        out_shape=(rim, rim, gain, gain, loss),
        in_specs=[pl.BlockSpec(memory_space=pltpu.VMEM)] + [anywhere] * 3,
        out_specs=(anywhere,) * 5,
        scratch_shapes=[pltpu.VMEM(rim.shape, f32)] * 2
        + [pltpu.VMEM(a.shape, f32) for a in (gains_a, gains_b, loss_rates)]
        + [pltpu.VMEM((COUNT, COUNT, LANES), f32)]
        + [pltpu.VMEM(a.shape, f32) for a in (gain, gain, loss)]
        + [dma((2,)), dma((2,)), dma((2, terms)), dma((2, terms)), dma, dma],
        compiler_params=pltpu.CompilerParams(collective_id=0, has_side_effects=True),
    )(density, gains_a, gains_b, loss_rates)


def rim_kernel(lower, upper, below, above, sends, receives):
    barrier, after, before = meet("gy")
    pl.semaphore_wait(barrier, 2)
    forth = passed(upper, below, after, sends, receives, 0)
    back = passed(lower, above, before, sends, receives, 1)
    forth.start()
    back.start()
    forth.wait()
    back.wait()


def rims(lower, upper):
    anywhere = pl.BlockSpec(memory_space=pl.ANY)
    rim = jax.ShapeDtypeStruct(lower.shape, f32)
    return pl.pallas_call(
        rim_kernel,
        out_shape=(rim, rim),
        in_specs=[anywhere] * 2,
        out_specs=(anywhere,) * 2,
        scratch_shapes=[pltpu.SemaphoreType.DMA((2,))] * 2,
        compiler_params=pltpu.CompilerParams(collective_id=1, has_side_effects=True),
    )(lower, upper)


def body(density, gains_a, gains_b, loss_rates):
    cells_x, count, merged = density.shape
    terms = gains_a.shape[0]
    groups = merged // (2 * count * count)
    below, above, *gains = start(density, gains_a, gains_b, loss_rates)
    tables = tuple(jnp.asarray(t) for t in transform_tables())
    inner = jax.ShapeDtypeStruct((4, PLACES, groups * LANES), f32)
    rim = jax.ShapeDtypeStruct((2, PLACES, LANES), f32)
    swept = pltpu.VMEM((2, 2, 16, merged), f32)
    field, lower, upper = call(
        x_kernel, groups, terms, (density, below, above, jnp.asarray(x_weights())), gains, tables, (inner, rim, rim), [swept]
    )
    below, above = rims(lower, upper)
    out = jax.ShapeDtypeStruct(density.shape, f32)
    return call(y_kernel, groups, terms, (field, below, above, jnp.asarray(y_weights())), gains, tables, out, [swept])


def solution(mesh):
    in_specs = (P("gx", None, "gy"), P(), P(), P())
    out_specs = P("gx", None, "gy")
    return jax.shard_map(body, mesh=mesh, in_specs=in_specs, out_specs=out_specs, check_vma=False)
```

```python
import functools

import jax
import jax.numpy as jnp
import numpy as np
from jax import lax
from jax.experimental import pallas as pl
from jax.experimental.pallas import tpu as pltpu
from jax.sharding import PartitionSpec as P

COUNT = 24
HALF = COUNT // 2
PLACES = HALF * HALF
LANES = 128
CELLS = 4
CHUNK = 16
THIRD = PLACES // 4
SPARE = LANES - CELLS * COUNT
collide_step = 0.2
courant_max = 1.6
f32 = jnp.float32


def cosine_table():
    freq = np.arange(COUNT)[:, None]
    points = np.arange(COUNT)[None, :]
    scale = np.where(freq == 0, np.sqrt(1.0 / COUNT), np.sqrt(2.0 / COUNT))
    return scale * np.cos(np.pi * (2 * points + 1) * freq / (2 * COUNT))


def two_parts(table):
    high = table.astype(jnp.bfloat16)
    return high, (table - high.astype(np.float64)).astype(jnp.bfloat16)


def transform_tables():
    cosine = cosine_table()
    plane = []
    for parity_x in range(2):
        for parity_y in range(2):
            along_x, along_y = cosine[parity_x::2, :HALF], cosine[parity_y::2, :HALF]
            plane.append(np.einsum("jn,lm->mnjl", along_x, along_y).reshape(PLACES, PLACES))
    plane = np.stack(plane)

    def stacked(table):
        return np.concatenate(two_parts(table), 1)

    def line(table):
        used = CELLS * COUNT
        wide = np.zeros((LANES, LANES))
        wide[:used, :used] = np.kron(np.eye(CELLS), table)
        high, low = two_parts(wide)
        return np.block([[high, low], [high, np.zeros_like(high)]])

    return stacked(plane.transpose(0, 2, 1)), line(cosine.T), stacked(plane), line(cosine)


def weights():
    speeds = np.arange(COUNT) - (COUNT - 1) / 2
    numbers = courant_max * np.abs(speeds) / ((COUNT - 1) / 2)
    return np.stack([1 - 1.5 * numbers + 0.5 * numbers**2, 2 * numbers - numbers**2, 0.5 * (numbers**2 - numbers)])


def x_weights():
    return np.broadcast_to(weights().reshape(3, 2, HALF, 1), (3, 2, HALF, LANES)).astype(np.float32)


def y_weights():
    both = weights().reshape(3, 2, HALF)
    both = np.stack([both[:, 0], both[:, 1, ::-1]], 1)
    both = np.repeat(both, HALF, 2)[..., None]
    return np.broadcast_to(both, (3, 2, PLACES, LANES)).astype(np.float32)


def split(value):
    high = value.astype(jnp.bfloat16)
    return high, (value - high.astype(f32)).astype(jnp.bfloat16)


def line_transform(value, table):
    both = jnp.dot(jnp.concatenate(split(value), 1), table, preferred_element_type=f32)
    return both[:, :LANES] + both[:, LANES:]


def plane_transform(value, table):
    high, low = split(value)
    first = jnp.dot(table, high, preferred_element_type=f32)
    second = jnp.dot(table[:PLACES], low, preferred_element_type=f32)
    return first[:PLACES] + first[PLACES:] + second


def butterfly(parts):
    sum_0, diff_0 = parts[0] + parts[1], parts[0] - parts[1]
    sum_1, diff_1 = parts[2] + parts[3], parts[2] - parts[3]
    return sum_0 + sum_1, diff_0 + diff_1, sum_0 - sum_1, diff_0 - diff_1


def block(index):
    return slice(index * LANES, (index + 1) * LANES)


def side_by_side(value, parts):
    return jnp.concatenate([value[i * PLACES : (i + 1) * PLACES] for i in range(parts)], 1)


def backward(groups, factors, modes, mixed, plane, line):
    parts = []
    for q in range(4):
        scaled = [modes[q, :, block(g)] * factor(q) for factor in factors for g in range(groups)]
        moved = plane_transform(jnp.concatenate(scaled, 1), plane[q])
        parts += [moved[:, block(i)] for i in range(len(scaled))]
    moved = line_transform(jnp.concatenate(parts, 0), line[...])
    count = len(factors) * groups
    for q in range(4):
        mixed[q, :, : count * LANES] = side_by_side(moved[q * count * PLACES : (q + 1) * count * PLACES], count)


def forward(groups, field, modes, mixed, plane, line):
    wide = groups * LANES
    for start in range(0, PLACES, CHUNK):
        rows = slice(start, start + CHUNK)
        parts = butterfly([field[q, rows, :] for q in range(4)])
        for q in range(4):
            mixed[q, rows, :wide] = parts[q]
    for q in range(4):
        moved = plane_transform(mixed[q, :, :wide], plane[q])
        stacked = jnp.concatenate([moved[:, block(g)] for g in range(groups)], 0)
        modes[q] = side_by_side(line_transform(stacked, line[...]), groups)


def collide(groups, field, total, modes, mixed, arrays, copies, loads, prepare):
    terms = copies[0].shape[0]
    wide = groups * LANES
    gain_a, gain_b, loss, plane_fwd, line_fwd, plane_back, line_back = copies

    def fixed(i):
        return pltpu.make_async_copy(arrays[i], copies[i], loads.at[2, i])

    def gain(i, p):
        return pltpu.make_async_copy(arrays[i].at[p], copies[i].at[p], loads.at[i, p])

    def load(p, carry):
        gain(0, p).start()
        gain(1, p).start()
        return carry

    for i in (3, 4, 2, 5, 6):
        fixed(i).start()
    lax.fori_loop(0, terms, load, 0)
    prepare()
    fixed(3).wait()
    fixed(4).wait()
    forward(groups, field, modes, mixed, plane_fwd, line_fwd)
    for i in (2, 5, 6):
        fixed(i).wait()
    backward(groups, [lambda q: loss[q]], modes, mixed, plane_back, line_back)
    for start in range(0, PLACES, CHUNK):
        rows = slice(start, start + CHUNK)
        parts = butterfly([mixed[q, rows, :wide] for q in range(4)])
        for q in range(4):
            total[q, rows, :] = -field[q, rows, :] * parts[q]

    def term(p, carry):
        gain(0, p).wait()
        gain(1, p).wait()
        backward(groups, [lambda q: gain_a[p, q], lambda q: gain_b[p, q]], modes, mixed, plane_back, line_back)
        for start in range(0, PLACES, CHUNK):
            rows = slice(start, start + CHUNK)
            first = butterfly([mixed[q, rows, :wide] for q in range(4)])
            second = butterfly([mixed[q, rows, wide : 2 * wide] for q in range(4)])
            for q in range(4):
                total[q, rows, :] += first[q] * second[q]
        return carry

    lax.fori_loop(0, terms, term, 0)


def piece(y, cell_x, cell_y):
    return cell_y * COUNT * COUNT + y * COUNT


def x_kernel(groups, density, below, above, weight, *refs):
    arrays, (out, lower, upper, swept, field, total, modes, mixed, *copies, loads) = refs[:7], refs[7:]

    def prepare():
        neg = [density[c, :HALF, :] for c in range(2)] + [above[:HALF, :], above[HALF:, :]]
        nw = [weight[k, 0, :, :1] for k in range(3)]
        for c in range(2):
            swept[c, 0, :HALF, :] = nw[0] * neg[c] + nw[1] * neg[c + 1] + nw[2] * neg[c + 2]
        pos = [below[:HALF, :], below[HALF:, :]] + [density[c, HALF:, :] for c in range(2)]
        pw = [weight[k, 1, :, :1] for k in range(3)]
        for c in range(2):
            new = pw[0] * pos[c + 2] + pw[1] * pos[c + 1] + pw[2] * pos[c]
            for row in range(HALF):
                swept[c, 1, HALF - 1 - row : HALF - row, :] = new[row : row + 1]
        for half_y in range(2):
            for place in range(HALF):
                y = COUNT - 1 - place if half_y else place
                for half_x in range(2):
                    for g in range(groups):
                        parts = []
                        for s in range(CELLS):
                            at = piece(y, s // 2, 2 * g + s % 2)
                            parts.append(swept[s // 2, half_x, :HALF, at : at + COUNT])
                        parts.append(jnp.zeros((HALF, LANES - CELLS * COUNT), f32))
                        field[2 * half_x + half_y, place * HALF : (place + 1) * HALF, block(g)] = jnp.concatenate(parts, 1)

    collide(groups, field, total, modes, mixed, arrays, copies, loads, prepare)

    for q in range(4):
        out[q] = field[q] + collide_step * total[q]
    for half_x in range(2):
        pack(out, 2 * half_x, block(0), lower, half_x)
        pack(out, 2 * half_x + 1, block(groups - 1), upper, half_x)


def pack(source, q, lanes, target, half_x):
    free = lax.broadcasted_iota(jnp.int32, (THIRD, LANES), 1) >= CELLS * COUNT
    rest = source[q, 3 * THIRD :, lanes]
    for k in range(3):
        kept = source[q, k * THIRD : (k + 1) * THIRD, lanes]
        start = (3 * half_x + k) * THIRD
        target[start : start + THIRD, :] = jnp.where(free, pltpu.roll(rest, CELLS * COUNT - k * SPARE, 1), kept)


def unpack(source, half_x, target):
    lane = lax.broadcasted_iota(jnp.int32, (THIRD, LANES), 1)
    rest = jnp.zeros((THIRD, LANES), f32)
    for k in range(3):
        start = (3 * half_x + k) * THIRD
        part = source[start : start + THIRD, :]
        target[k * THIRD : (k + 1) * THIRD, :] = jnp.where(lane < CELLS * COUNT, part, 0.0)
        rest = jnp.where(lane // SPARE == k, pltpu.roll(part, LANES - CELLS * COUNT + k * SPARE, 1), rest)
    target[3 * THIRD :, :] = rest


def y_kernel(groups, before, below, above, weight, *refs):
    arrays, (out, swept, rim, field, total, modes, mixed, *copies, loads) = refs[:7], refs[7:]

    def prepare():
        place = lax.broadcasted_iota(jnp.int32, (PLACES, LANES), 1) // COUNT
        odd = place % 2 == 1
        for half_x in range(2):
            for half_y in range(2):
                q = 2 * half_x + half_y
                w0, w1, w2 = [weight[k, half_y] for k in range(3)]
                blocks = [before[q, :, block(g)] for g in range(groups)]
                unpack(below if half_y else above, half_x, rim)
                blocks = [rim[...]] + blocks if half_y else blocks + [rim[...]]
                right = [pltpu.roll(b, COUNT, 1) for b in blocks]
                left = [pltpu.roll(b, LANES - COUNT, 1) for b in blocks]
                for g in range(groups):
                    if half_y:
                        near = jnp.where(odd, right[g + 1], left[g])
                        new = w0 * blocks[g + 1] + w1 * near + w2 * blocks[g]
                    else:
                        near = jnp.where(odd, right[g + 1], left[g])
                        new = w0 * blocks[g] + w1 * near + w2 * blocks[g + 1]
                    field[q, :, block(g)] = new

    collide(groups, field, total, modes, mixed, arrays, copies, loads, prepare)

    for q in range(4):
        field[q] = field[q] + collide_step * total[q]
    for half_x in range(2):
        for c in range(2):
            for g in range(groups):
                parts = []
                for cell_y in range(2):
                    for y in range(COUNT):
                        half_y, place = (0, y) if y < HALF else (1, COUNT - 1 - y)
                        at = g * LANES + (2 * c + cell_y) * COUNT
                        parts.append(field[2 * half_x + half_y, place * HALF : (place + 1) * HALF, at : at + COUNT])
                wide = 2 * COUNT * COUNT
                swept[c, half_x, :HALF, g * wide : (g + 1) * wide] = jnp.concatenate(parts, 1)
    for c in range(2):
        out[c, :HALF, :] = swept[c, 0, :HALF, :]
        for row in range(HALF):
            out[c, HALF + row : HALF + row + 1, :] = swept[c, 1, HALF - 1 - row : HALF - row, :]


def call(kernel, groups, field_args, arrays, out_shapes, scratch):
    wide = groups * LANES
    inside = pl.BlockSpec(memory_space=pltpu.VMEM)
    terms = arrays[0].shape[0]
    return pl.pallas_call(
        functools.partial(kernel, groups),
        out_shape=out_shapes,
        in_specs=[inside] * len(field_args) + [pl.BlockSpec(memory_space=pl.ANY)] * len(arrays),
        out_specs=jax.tree.map(lambda _: inside, out_shapes),
        scratch_shapes=scratch
        + [pltpu.VMEM((4, PLACES, n * wide), f32) for n in (1, 1, 1, 2)]
        + [pltpu.VMEM(a.shape, a.dtype) for a in arrays]
        + [pltpu.SemaphoreType.DMA((3, max(terms, len(arrays))))],
    )(*field_args, *arrays)


def meet(axis):
    count = lax.axis_size(axis)
    me = lax.axis_index(axis)
    after, before = {axis: lax.rem(me + 1, count)}, {axis: lax.rem(me + count - 1, count)}
    barrier = pltpu.get_barrier_semaphore()
    for neighbour in (after, before):
        pl.semaphore_signal(barrier, inc=1, device_id=neighbour, device_id_type=pl.DeviceIdType.MESH)
    return barrier, after, before


def passed(source, target, device, sends, receives, index):
    return pltpu.make_async_remote_copy(
        src_ref=source,
        dst_ref=target,
        send_sem=sends.at[index],
        recv_sem=receives.at[index],
        device_id=device,
        device_id_type=pl.DeviceIdType.MESH,
    )


def spread(raw, wide, out):
    used = lax.broadcasted_iota(jnp.int32, (COUNT, LANES), 1) < COUNT
    for mode in range(COUNT):
        value = jnp.concatenate([raw[mode], jnp.zeros((COUNT, LANES - COUNT), f32)], 1)
        value = jnp.where(used, value, 0.0)
        value = value + pltpu.roll(value, COUNT, 1)
        wide[mode] = value + pltpu.roll(value, 2 * COUNT, 1)
    for parity_x in range(2):
        for parity_y in range(2):
            rows = [wide[2 * place + parity_x, pl.ds(parity_y, HALF, stride=2), :] for place in range(HALF)]
            for place in range(0, HALF, 2):
                out[2 * parity_x + parity_y, place * HALF : (place + 2) * HALF, :] = jnp.concatenate(rows[place : place + 2], 0)


def start_kernel(density, gain_a, gain_b, loss, below, above, out_a, out_b, out_loss, *refs):
    up, down, raw_a, raw_b, raw_loss, wide, made_a, made_b, made_loss, sends, receives, loads, saves, load_loss, save_loss = refs
    terms = raw_a.shape[0]
    sides = ((0, gain_a, raw_a, made_a, out_a), (1, gain_b, raw_b, made_b, out_b))

    def load(p, side):
        i, source, raw, _, _ = sides[side]
        return pltpu.make_async_copy(source.at[p], raw.at[p], loads.at[i, p])

    def save(p, side):
        i, _, _, made, out = sides[side]
        return pltpu.make_async_copy(made.at[p], out.at[p], saves.at[i, p])

    pltpu.make_async_copy(loss, raw_loss, load_loss).start()
    for side in range(2):
        lax.fori_loop(0, terms, lambda p, c: (load(p, side).start(), c)[1], 0)
    barrier, after, before = meet("gx")
    for c in range(2):
        up[c * HALF : (c + 1) * HALF, :] = density[c, HALF:, :]
        down[c * HALF : (c + 1) * HALF, :] = density[c, :HALF, :]
    pl.semaphore_wait(barrier, 2)
    forth = passed(up, below, after, sends, receives, 0)
    back = passed(down, above, before, sends, receives, 1)
    forth.start()
    back.start()
    pltpu.make_async_copy(loss, raw_loss, load_loss).wait()
    spread(raw_loss, wide, made_loss)
    pltpu.make_async_copy(made_loss, out_loss, save_loss).start()
    for side in range(2):

        def one(p, carry):
            load(p, side).wait()
            spread(sides[side][2].at[p], wide, sides[side][3].at[p])
            save(p, side).start()
            return carry

        lax.fori_loop(0, terms, one, 0)
    for side in range(2):
        lax.fori_loop(0, terms, lambda p, c: (save(p, side).wait(), c)[1], 0)
    pltpu.make_async_copy(made_loss, out_loss, save_loss).wait()
    forth.wait()
    back.wait()


def start(density, gains_a, gains_b, loss_rates):
    terms = gains_a.shape[0]
    rim = jax.ShapeDtypeStruct((COUNT, density.shape[2]), f32)
    gain = jax.ShapeDtypeStruct((terms, 4, PLACES, LANES), f32)
    loss = jax.ShapeDtypeStruct((4, PLACES, LANES), f32)
    anywhere = pl.BlockSpec(memory_space=pl.ANY)
    dma = pltpu.SemaphoreType.DMA
    return pl.pallas_call(
        start_kernel,
        out_shape=(rim, rim, gain, gain, loss),
        in_specs=[pl.BlockSpec(memory_space=pltpu.VMEM)] + [anywhere] * 3,
        out_specs=(anywhere,) * 5,
        scratch_shapes=[pltpu.VMEM(rim.shape, f32)] * 2
        + [pltpu.VMEM(a.shape, f32) for a in (gains_a, gains_b, loss_rates)]
        + [pltpu.VMEM((COUNT, COUNT, LANES), f32)]
        + [pltpu.VMEM(a.shape, f32) for a in (gain, gain, loss)]
        + [dma((2,)), dma((2,)), dma((2, terms)), dma((2, terms)), dma, dma],
        compiler_params=pltpu.CompilerParams(collective_id=0, has_side_effects=True),
    )(density, gains_a, gains_b, loss_rates)


def rim_kernel(lower, upper, below, above, sends, receives):
    barrier, after, before = meet("gy")
    pl.semaphore_wait(barrier, 2)
    forth = passed(upper, below, after, sends, receives, 0)
    back = passed(lower, above, before, sends, receives, 1)
    forth.start()
    back.start()
    forth.wait()
    back.wait()


def rims(lower, upper):
    anywhere = pl.BlockSpec(memory_space=pl.ANY)
    rim = jax.ShapeDtypeStruct(lower.shape, f32)
    return pl.pallas_call(
        rim_kernel,
        out_shape=(rim, rim),
        in_specs=[anywhere] * 2,
        out_specs=(anywhere,) * 2,
        scratch_shapes=[pltpu.SemaphoreType.DMA((2,))] * 2,
        compiler_params=pltpu.CompilerParams(collective_id=1, has_side_effects=True),
    )(lower, upper)


def body(density, gains_a, gains_b, loss_rates):
    count, merged = density.shape[1:]
    groups = merged // (2 * count * count)
    below, above, *gains = start(density, gains_a, gains_b, loss_rates)
    arrays = (*gains, *[jnp.asarray(t) for t in transform_tables()])
    inner = jax.ShapeDtypeStruct((4, PLACES, groups * LANES), f32)
    rim = jax.ShapeDtypeStruct((6 * THIRD, LANES), f32)
    swept = pltpu.VMEM((2, 2, 16, merged), f32)
    field, lower, upper = call(
        x_kernel, groups, (density, below, above, jnp.asarray(x_weights())), arrays, (inner, rim, rim), [swept]
    )
    below, above = rims(lower, upper)
    out = jax.ShapeDtypeStruct(density.shape, f32)
    return call(y_kernel, groups, (field, below, above, jnp.asarray(y_weights())), arrays, out, [swept, pltpu.VMEM((PLACES, LANES), f32)])


def solution(mesh):
    in_specs = (P("gx", None, "gy"), P(), P(), P())
    out_specs = P("gx", None, "gy")
    return jax.shard_map(body, mesh=mesh, in_specs=in_specs, out_specs=out_specs, check_vma=False)
```

```python
import functools

import jax
import jax.numpy as jnp
import numpy as np
from jax import lax
from jax.experimental import pallas as pl
from jax.experimental.pallas import tpu as pltpu
from jax.sharding import PartitionSpec as P

COUNT = 24
HALF = COUNT // 2
PLACES = HALF * HALF
LANES = 128
CELLS = 4
CHUNK = 16
THIRD = PLACES // 4
SPARE = LANES - CELLS * COUNT
collide_step = 0.2
courant_max = 1.6
f32 = jnp.float32


def cosine_table():
    freq = np.arange(COUNT)[:, None]
    points = np.arange(COUNT)[None, :]
    scale = np.where(freq == 0, np.sqrt(1.0 / COUNT), np.sqrt(2.0 / COUNT))
    return scale * np.cos(np.pi * (2 * points + 1) * freq / (2 * COUNT))


def two_parts(table):
    high = table.astype(jnp.bfloat16)
    return high, (table - high.astype(np.float64)).astype(jnp.bfloat16)


def transform_tables():
    cosine = cosine_table()
    plane = []
    for parity_x in range(2):
        for parity_y in range(2):
            along_x, along_y = cosine[parity_x::2, :HALF], cosine[parity_y::2, :HALF]
            plane.append(np.einsum("jn,lm->mnjl", along_x, along_y).reshape(PLACES, PLACES))
    plane = np.stack(plane)

    def stacked(table):
        return np.concatenate(two_parts(table), 1)

    def line(table):
        used = CELLS * COUNT
        wide = np.zeros((LANES, LANES))
        wide[:used, :used] = np.kron(np.eye(CELLS), table)
        high, low = two_parts(wide)
        return np.block([[high, low], [high, np.zeros_like(high)]])

    return stacked(plane.transpose(0, 2, 1)), line(cosine.T), stacked(plane), line(cosine)


def weights():
    speeds = np.arange(COUNT) - (COUNT - 1) / 2
    numbers = courant_max * np.abs(speeds) / ((COUNT - 1) / 2)
    return np.stack([1 - 1.5 * numbers + 0.5 * numbers**2, 2 * numbers - numbers**2, 0.5 * (numbers**2 - numbers)])


def x_weights():
    return np.broadcast_to(weights().reshape(3, 2, HALF, 1), (3, 2, HALF, LANES)).astype(np.float32)


def y_weights():
    both = weights().reshape(3, 2, HALF)
    both = np.stack([both[:, 0], both[:, 1, ::-1]], 1)
    both = np.repeat(both, HALF, 2)[..., None]
    return np.broadcast_to(both, (3, 2, PLACES, LANES)).astype(np.float32)


def split(value):
    high = value.astype(jnp.bfloat16)
    return high, (value - high.astype(f32)).astype(jnp.bfloat16)


def line_transform(value, table):
    both = jnp.dot(jnp.concatenate(split(value), 1), table, preferred_element_type=f32)
    return both[:, :LANES] + both[:, LANES:]


def plane_transform(value, table):
    high, low = split(value)
    first = jnp.dot(table, high, preferred_element_type=f32)
    second = jnp.dot(table[:PLACES], low, preferred_element_type=f32)
    return first[:PLACES] + first[PLACES:] + second


def butterfly(parts):
    sum_0, diff_0 = parts[0] + parts[1], parts[0] - parts[1]
    sum_1, diff_1 = parts[2] + parts[3], parts[2] - parts[3]
    return sum_0 + sum_1, diff_0 + diff_1, sum_0 - sum_1, diff_0 - diff_1


def block(index):
    return slice(index * LANES, (index + 1) * LANES)


def side_by_side(value, parts):
    return jnp.concatenate([value[i * PLACES : (i + 1) * PLACES] for i in range(parts)], 1)


def backward(groups, factors, modes, mixed, plane, line):
    parts = []
    for q in range(4):
        scaled = [modes[q, :, block(g)] * factor(q) for factor in factors for g in range(groups)]
        moved = plane_transform(jnp.concatenate(scaled, 1), plane[q])
        parts += [moved[:, block(i)] for i in range(len(scaled))]
    moved = line_transform(jnp.concatenate(parts, 0), line[...])
    count = len(factors) * groups
    for q in range(4):
        mixed[q, :, : count * LANES] = side_by_side(moved[q * count * PLACES : (q + 1) * count * PLACES], count)


def forward(groups, field, modes, mixed, plane, line):
    wide = groups * LANES
    for start in range(0, PLACES, CHUNK):
        rows = slice(start, start + CHUNK)
        parts = butterfly([field[q, rows, :] for q in range(4)])
        for q in range(4):
            mixed[q, rows, :wide] = parts[q]
    for q in range(4):
        moved = plane_transform(mixed[q, :, :wide], plane[q])
        stacked = jnp.concatenate([moved[:, block(g)] for g in range(groups)], 0)
        modes[q] = side_by_side(line_transform(stacked, line[...]), groups)


def collide(groups, field, total, modes, mixed, arrays, copies, loads, prepare):
    terms = copies[0].shape[0]
    wide = groups * LANES
    gain_a, gain_b, loss, plane_fwd, line_fwd, plane_back, line_back = copies

    def fixed(i):
        return pltpu.make_async_copy(arrays[i], copies[i], loads.at[2, i])

    def gain(i, p):
        return pltpu.make_async_copy(arrays[i].at[p], copies[i].at[p], loads.at[i, p])

    def load(p, carry):
        gain(0, p).start()
        gain(1, p).start()
        return carry

    for i in (3, 4, 2, 5, 6):
        fixed(i).start()
    lax.fori_loop(0, terms, load, 0)
    prepare()
    fixed(3).wait()
    fixed(4).wait()
    forward(groups, field, modes, mixed, plane_fwd, line_fwd)
    for i in (2, 5, 6):
        fixed(i).wait()
    backward(groups, [lambda q: loss[q]], modes, mixed, plane_back, line_back)
    for start in range(0, PLACES, CHUNK):
        rows = slice(start, start + CHUNK)
        parts = butterfly([mixed[q, rows, :wide] for q in range(4)])
        for q in range(4):
            total[q, rows, :] = -field[q, rows, :] * parts[q]

    def term(p, carry):
        gain(0, p).wait()
        gain(1, p).wait()
        backward(groups, [lambda q: gain_a[p, q], lambda q: gain_b[p, q]], modes, mixed, plane_back, line_back)
        for start in range(0, PLACES, CHUNK):
            rows = slice(start, start + CHUNK)
            first = butterfly([mixed[q, rows, :wide] for q in range(4)])
            second = butterfly([mixed[q, rows, wide : 2 * wide] for q in range(4)])
            for q in range(4):
                total[q, rows, :] += first[q] * second[q]
        return carry

    lax.fori_loop(0, terms, term, 0)


def piece(y, cell_x, cell_y):
    return cell_y * COUNT * COUNT + y * COUNT


def x_kernel(groups, density, ghost_below, ghost_above, weight, *refs):
    arrays, (out, rim_below, rim_above, swept, lower, upper, sends, receives, save), rest = refs[:7], refs[7:16], refs[16:]
    field, total, modes, mixed, *copies, loads = rest
    barrier, after, before = meet("gy")

    def prepare():
        neg = [density[c, :HALF, :] for c in range(2)] + [ghost_above[:HALF, :], ghost_above[HALF:, :]]
        nw = [weight[k, 0, :, :1] for k in range(3)]
        for c in range(2):
            swept[c, :HALF, :] = nw[0] * neg[c] + nw[1] * neg[c + 1] + nw[2] * neg[c + 2]
        pos = [ghost_below[:HALF, :], ghost_below[HALF:, :]] + [density[c, HALF:, :] for c in range(2)]
        pw = [weight[k, 1, :, :1] for k in range(3)]
        for c in range(2):
            new = pw[0] * pos[c + 2] + pw[1] * pos[c + 1] + pw[2] * pos[c]
            for row in range(HALF):
                swept[c, COUNT - 1 - row : COUNT - row, :] = new[row : row + 1]
        for half_y in range(2):
            for place in range(HALF):
                y = COUNT - 1 - place if half_y else place
                for g in range(groups):
                    parts = []
                    for s in range(CELLS):
                        at = piece(y, s // 2, 2 * g + s % 2)
                        parts.append(swept[s // 2, :, at : at + COUNT])
                    parts.append(jnp.zeros((COUNT, LANES - CELLS * COUNT), f32))
                    moved = jnp.concatenate(parts, 1)
                    rows = slice(place * HALF, (place + 1) * HALF)
                    field[half_y, rows, block(g)] = moved[:HALF]
                    field[2 + half_y, rows, block(g)] = moved[HALF:]

    collide(groups, field, total, modes, mixed, arrays, copies, loads, prepare)

    for q in range(4):
        field[q] = field[q] + collide_step * total[q]
    for half_x in range(2):
        pack(field, 2 * half_x, block(0), lower, half_x)
        pack(field, 2 * half_x + 1, block(groups - 1), upper, half_x)
    pl.semaphore_wait(barrier, 2)
    forth = passed(upper, rim_below, after, sends, receives, 0)
    back = passed(lower, rim_above, before, sends, receives, 1)
    forth.start()
    back.start()
    whole = pltpu.make_async_copy(field, out, save)
    whole.start()
    whole.wait()
    forth.wait()
    back.wait()


def pack(source, q, lanes, target, half_x):
    free = lax.broadcasted_iota(jnp.int32, (THIRD, LANES), 1) >= CELLS * COUNT
    rest = source[q, 3 * THIRD :, lanes]
    for k in range(3):
        kept = source[q, k * THIRD : (k + 1) * THIRD, lanes]
        start = (3 * half_x + k) * THIRD
        target[start : start + THIRD, :] = jnp.where(free, pltpu.roll(rest, CELLS * COUNT - k * SPARE, 1), kept)


def unpack(source, half_x, target):
    lane = lax.broadcasted_iota(jnp.int32, (THIRD, LANES), 1)
    rest = jnp.zeros((THIRD, LANES), f32)
    for k in range(3):
        start = (3 * half_x + k) * THIRD
        part = source[start : start + THIRD, :]
        target[k * THIRD : (k + 1) * THIRD, :] = jnp.where(lane < CELLS * COUNT, part, 0.0)
        rest = jnp.where(lane // SPARE == k, pltpu.roll(part, LANES - CELLS * COUNT + k * SPARE, 1), rest)
    target[3 * THIRD :, :] = rest


def y_kernel(groups, before, below, above, weight, *refs):
    arrays, (out, swept, rim, field, total, modes, mixed, *copies, loads) = refs[:7], refs[7:]

    def prepare():
        place = lax.broadcasted_iota(jnp.int32, (PLACES, LANES), 1) // COUNT
        odd = place % 2 == 1
        for half_x in range(2):
            for half_y in range(2):
                q = 2 * half_x + half_y
                w0, w1, w2 = [weight[k, half_y] for k in range(3)]
                blocks = [before[q, :, block(g)] for g in range(groups)]
                unpack(below if half_y else above, half_x, rim)
                blocks = [rim[...]] + blocks if half_y else blocks + [rim[...]]
                right = [pltpu.roll(b, COUNT, 1) for b in blocks]
                left = [pltpu.roll(b, LANES - COUNT, 1) for b in blocks]
                for g in range(groups):
                    if half_y:
                        near = jnp.where(odd, right[g + 1], left[g])
                        new = w0 * blocks[g + 1] + w1 * near + w2 * blocks[g]
                    else:
                        near = jnp.where(odd, right[g + 1], left[g])
                        new = w0 * blocks[g] + w1 * near + w2 * blocks[g + 1]
                    field[q, :, block(g)] = new

    collide(groups, field, total, modes, mixed, arrays, copies, loads, prepare)

    for q in range(4):
        field[q] = field[q] + collide_step * total[q]
    wide = 2 * COUNT * COUNT
    for g in range(groups):
        columns = []
        for y in range(COUNT):
            half_y, place = (0, y) if y < HALF else (1, COUNT - 1 - y)
            rows = slice(place * HALF, (place + 1) * HALF)
            columns.append(jnp.concatenate([field[half_y, rows, block(g)], field[2 + half_y, rows, block(g)]], 0))
        for c in range(2):
            parts = []
            for cell_y in range(2):
                at = (2 * c + cell_y) * COUNT
                parts += [column[:, at : at + COUNT] for column in columns]
            swept[c, :, g * wide : (g + 1) * wide] = jnp.concatenate(parts, 1)
    for c in range(2):
        out[c, :HALF, :] = swept[c, :HALF, :]
        for row in range(HALF):
            out[c, HALF + row : HALF + row + 1, :] = swept[c, COUNT - 1 - row : COUNT - row, :]


def call(kernel, groups, field_args, arrays, out_shapes, out_space, scratch, **settings):
    wide = groups * LANES
    inside = pl.BlockSpec(memory_space=pltpu.VMEM)
    terms = arrays[0].shape[0]
    return pl.pallas_call(
        functools.partial(kernel, groups),
        out_shape=out_shapes,
        in_specs=[inside] * len(field_args) + [pl.BlockSpec(memory_space=pl.ANY)] * len(arrays),
        out_specs=jax.tree.map(lambda _: pl.BlockSpec(memory_space=out_space), out_shapes),
        compiler_params=pltpu.CompilerParams(**settings),
        scratch_shapes=scratch
        + [pltpu.VMEM((4, PLACES, n * wide), f32) for n in (1, 1, 1, 2)]
        + [pltpu.VMEM(a.shape, a.dtype) for a in arrays]
        + [pltpu.SemaphoreType.DMA((3, max(terms, len(arrays))))],
    )(*field_args, *arrays)


def meet(axis):
    count = lax.axis_size(axis)
    me = lax.axis_index(axis)
    after, before = {axis: lax.rem(me + 1, count)}, {axis: lax.rem(me + count - 1, count)}
    barrier = pltpu.get_barrier_semaphore()
    for neighbour in (after, before):
        pl.semaphore_signal(barrier, inc=1, device_id=neighbour, device_id_type=pl.DeviceIdType.MESH)
    return barrier, after, before


def passed(source, target, device, sends, receives, index):
    return pltpu.make_async_remote_copy(
        src_ref=source,
        dst_ref=target,
        send_sem=sends.at[index],
        recv_sem=receives.at[index],
        device_id=device,
        device_id_type=pl.DeviceIdType.MESH,
    )


def spread(raw, wide, out):
    used = lax.broadcasted_iota(jnp.int32, (COUNT, LANES), 1) < COUNT
    for mode in range(COUNT):
        value = jnp.concatenate([raw[mode], jnp.zeros((COUNT, LANES - COUNT), f32)], 1)
        value = jnp.where(used, value, 0.0)
        value = value + pltpu.roll(value, COUNT, 1)
        wide[mode] = value + pltpu.roll(value, 2 * COUNT, 1)
    for parity_x in range(2):
        for parity_y in range(2):
            rows = [wide[2 * place + parity_x, pl.ds(parity_y, HALF, stride=2), :] for place in range(HALF)]
            for place in range(0, HALF, 2):
                out[2 * parity_x + parity_y, place * HALF : (place + 2) * HALF, :] = jnp.concatenate(rows[place : place + 2], 0)


def start_kernel(density, gain_a, gain_b, loss, below, above, out_a, out_b, out_loss, *refs):
    up, down, raw_a, raw_b, raw_loss, wide, made_a, made_b, made_loss, sends, receives, loads, saves, load_loss, save_loss = refs
    terms = raw_a.shape[0]
    sides = ((0, gain_a, raw_a, made_a, out_a), (1, gain_b, raw_b, made_b, out_b))

    def load(p, side):
        i, source, raw, _, _ = sides[side]
        return pltpu.make_async_copy(source.at[p], raw.at[p], loads.at[i, p])

    def save(p, side):
        i, _, _, made, out = sides[side]
        return pltpu.make_async_copy(made.at[p], out.at[p], saves.at[i, p])

    pltpu.make_async_copy(loss, raw_loss, load_loss).start()
    for side in range(2):
        lax.fori_loop(0, terms, lambda p, c: (load(p, side).start(), c)[1], 0)
    barrier, after, before = meet("gx")
    for c in range(2):
        up[c * HALF : (c + 1) * HALF, :] = density[c, HALF:, :]
        down[c * HALF : (c + 1) * HALF, :] = density[c, :HALF, :]
    pl.semaphore_wait(barrier, 2)
    forth = passed(up, below, after, sends, receives, 0)
    back = passed(down, above, before, sends, receives, 1)
    forth.start()
    back.start()
    pltpu.make_async_copy(loss, raw_loss, load_loss).wait()
    spread(raw_loss, wide, made_loss)
    pltpu.make_async_copy(made_loss, out_loss, save_loss).start()
    for side in range(2):

        def one(p, carry):
            load(p, side).wait()
            spread(sides[side][2].at[p], wide, sides[side][3].at[p])
            save(p, side).start()
            return carry

        lax.fori_loop(0, terms, one, 0)
    for side in range(2):
        lax.fori_loop(0, terms, lambda p, c: (save(p, side).wait(), c)[1], 0)
    pltpu.make_async_copy(made_loss, out_loss, save_loss).wait()
    forth.wait()
    back.wait()


def start(density, gains_a, gains_b, loss_rates):
    terms = gains_a.shape[0]
    rim = jax.ShapeDtypeStruct((COUNT, density.shape[2]), f32)
    gain = jax.ShapeDtypeStruct((terms, 4, PLACES, LANES), f32)
    loss = jax.ShapeDtypeStruct((4, PLACES, LANES), f32)
    anywhere = pl.BlockSpec(memory_space=pl.ANY)
    dma = pltpu.SemaphoreType.DMA
    return pl.pallas_call(
        start_kernel,
        out_shape=(rim, rim, gain, gain, loss),
        in_specs=[pl.BlockSpec(memory_space=pltpu.VMEM)] + [anywhere] * 3,
        out_specs=(anywhere,) * 5,
        scratch_shapes=[pltpu.VMEM(rim.shape, f32)] * 2
        + [pltpu.VMEM(a.shape, f32) for a in (gains_a, gains_b, loss_rates)]
        + [pltpu.VMEM((COUNT + 1, COUNT, LANES), f32)]
        + [pltpu.VMEM(a.shape, f32) for a in (gain, gain, loss)]
        + [dma((2,)), dma((2,)), dma((2, terms)), dma((2, terms)), dma, dma],
        compiler_params=pltpu.CompilerParams(collective_id=0, has_side_effects=True),
    )(density, gains_a, gains_b, loss_rates)


def body(density, gains_a, gains_b, loss_rates):
    count, merged = density.shape[1:]
    groups = merged // (2 * count * count)
    below, above, *gains = start(density, gains_a, gains_b, loss_rates)
    arrays = (*gains, *[jnp.asarray(t) for t in transform_tables()])
    inner = jax.ShapeDtypeStruct((4, PLACES, groups * LANES), f32)
    rim = jax.ShapeDtypeStruct((6 * THIRD, LANES), f32)
    swept = pltpu.VMEM((2, count, merged), f32)
    dma = pltpu.SemaphoreType.DMA
    rims = [pltpu.VMEM(rim.shape, f32)] * 2 + [dma((2,)), dma((2,)), dma]
    before = (density, below, above, jnp.asarray(x_weights()))
    settings = dict(collective_id=1, has_side_effects=True)
    field, below, above = call(x_kernel, groups, before, arrays, (inner, rim, rim), pl.ANY, [swept] + rims, **settings)
    out = jax.ShapeDtypeStruct(density.shape, f32)
    return call(y_kernel, groups, (field, below, above, jnp.asarray(y_weights())), arrays, out, pltpu.VMEM, [swept, pltpu.VMEM((PLACES, LANES), f32)])


def solution(mesh):
    in_specs = (P("gx", None, "gy"), P(), P(), P())
    out_specs = P("gx", None, "gy")
    return jax.shard_map(body, mesh=mesh, in_specs=in_specs, out_specs=out_specs, check_vma=False)
```

```python
import functools

import jax
import jax.numpy as jnp
import numpy as np
from jax import lax
from jax.experimental import pallas as pl
from jax.experimental.pallas import tpu as pltpu
from jax.sharding import PartitionSpec as P

COUNT = 24
HALF = COUNT // 2
PLACES = HALF * HALF
LANES = 128
CELLS = 4
CHUNK = 16
THIRD = PLACES // 4
SPARE = LANES - CELLS * COUNT
collide_step = 0.2
courant_max = 1.6
f32 = jnp.float32


def cosine_table():
    freq = np.arange(COUNT)[:, None]
    points = np.arange(COUNT)[None, :]
    scale = np.where(freq == 0, np.sqrt(1.0 / COUNT), np.sqrt(2.0 / COUNT))
    return scale * np.cos(np.pi * (2 * points + 1) * freq / (2 * COUNT))


def two_parts(table):
    high = table.astype(jnp.bfloat16)
    return high, (table - high.astype(np.float64)).astype(jnp.bfloat16)


def transform_tables():
    cosine = cosine_table()
    plane = []
    for parity_x in range(2):
        for parity_y in range(2):
            along_x, along_y = cosine[parity_x::2, :HALF], cosine[parity_y::2, :HALF]
            plane.append(np.einsum("jn,lm->mnjl", along_x, along_y).reshape(PLACES, PLACES))
    plane = np.stack(plane)

    def stacked(table):
        return np.concatenate(two_parts(table), 1)

    def line(table):
        used = CELLS * COUNT
        wide = np.zeros((LANES, LANES))
        wide[:used, :used] = np.kron(np.eye(CELLS), table)
        high, low = two_parts(wide)
        return np.block([[high, low], [high, np.zeros_like(high)]])

    return stacked(plane.transpose(0, 2, 1)), line(cosine.T), stacked(plane), line(cosine)


def weights():
    speeds = np.arange(COUNT) - (COUNT - 1) / 2
    numbers = courant_max * np.abs(speeds) / ((COUNT - 1) / 2)
    return np.stack([1 - 1.5 * numbers + 0.5 * numbers**2, 2 * numbers - numbers**2, 0.5 * (numbers**2 - numbers)])


def x_weights():
    return np.broadcast_to(weights().reshape(3, 2, HALF, 1), (3, 2, HALF, LANES)).astype(np.float32)


def y_weights():
    both = weights().reshape(3, 2, HALF)
    both = np.stack([both[:, 0], both[:, 1, ::-1]], 1)
    both = np.repeat(both, HALF, 2)[..., None]
    return np.broadcast_to(both, (3, 2, PLACES, LANES)).astype(np.float32)


def split(value):
    high = value.astype(jnp.bfloat16)
    return high, (value - high.astype(f32)).astype(jnp.bfloat16)


def line_transform(value, table):
    both = jnp.dot(jnp.concatenate(split(value), 1), table, preferred_element_type=f32)
    return both[:, :LANES] + both[:, LANES:]


def plane_transform(value, table):
    high, low = split(value)
    first = jnp.dot(table, high, preferred_element_type=f32)
    second = jnp.dot(table[:PLACES], low, preferred_element_type=f32)
    return first[:PLACES] + first[PLACES:] + second


def butterfly(parts):
    sum_0, diff_0 = parts[0] + parts[1], parts[0] - parts[1]
    sum_1, diff_1 = parts[2] + parts[3], parts[2] - parts[3]
    return sum_0 + sum_1, diff_0 + diff_1, sum_0 - sum_1, diff_0 - diff_1


def block(index):
    return slice(index * LANES, (index + 1) * LANES)


def side_by_side(value, parts):
    return jnp.concatenate([value[i * PLACES : (i + 1) * PLACES] for i in range(parts)], 1)


def backward(groups, factors, modes, mixed, plane, line):
    parts = []
    for q in range(4):
        scaled = [modes[q, :, block(g)] * factor(q) for factor in factors for g in range(groups)]
        moved = plane_transform(jnp.concatenate(scaled, 1), plane[q])
        parts += [moved[:, block(i)] for i in range(len(scaled))]
    moved = line_transform(jnp.concatenate(parts, 0), line[...])
    count = len(factors) * groups
    for q in range(4):
        mixed[q, :, : count * LANES] = side_by_side(moved[q * count * PLACES : (q + 1) * count * PLACES], count)


def forward(groups, field, modes, mixed, plane, line):
    wide = groups * LANES
    for start in range(0, PLACES, CHUNK):
        rows = slice(start, start + CHUNK)
        parts = butterfly([field[q, rows, :] for q in range(4)])
        for q in range(4):
            mixed[q, rows, :wide] = parts[q]
    for q in range(4):
        moved = plane_transform(mixed[q, :, :wide], plane[q])
        stacked = jnp.concatenate([moved[:, block(g)] for g in range(groups)], 0)
        modes[q] = side_by_side(line_transform(stacked, line[...]), groups)


def collide(groups, field, total, modes, mixed, arrays, copies, loads, prepare):
    terms = copies[0].shape[0]
    wide = groups * LANES
    gain_a, gain_b, loss, plane_fwd, line_fwd, plane_back, line_back = copies

    def fixed(i):
        return pltpu.make_async_copy(arrays[i], copies[i], loads.at[2, i])

    def gain(i, p):
        return pltpu.make_async_copy(arrays[i].at[p], copies[i].at[p], loads.at[i, p])

    def load(p, carry):
        gain(0, p).start()
        gain(1, p).start()
        return carry

    for i in (3, 4, 2, 5, 6):
        fixed(i).start()
    lax.fori_loop(0, terms, load, 0)
    prepare()
    fixed(3).wait()
    fixed(4).wait()
    forward(groups, field, modes, mixed, plane_fwd, line_fwd)
    for i in (2, 5, 6):
        fixed(i).wait()
    backward(groups, [lambda q: loss[q]], modes, mixed, plane_back, line_back)
    for start in range(0, PLACES, CHUNK):
        rows = slice(start, start + CHUNK)
        parts = butterfly([mixed[q, rows, :wide] for q in range(4)])
        for q in range(4):
            total[q, rows, :] = -field[q, rows, :] * parts[q]

    def term(p, carry):
        gain(0, p).wait()
        gain(1, p).wait()
        backward(groups, [lambda q: gain_a[p, q], lambda q: gain_b[p, q]], modes, mixed, plane_back, line_back)
        for start in range(0, PLACES, CHUNK):
            rows = slice(start, start + CHUNK)
            first = butterfly([mixed[q, rows, :wide] for q in range(4)])
            second = butterfly([mixed[q, rows, wide : 2 * wide] for q in range(4)])
            for q in range(4):
                total[q, rows, :] += first[q] * second[q]
        return carry

    lax.fori_loop(0, terms, term, 0)


def piece(y, cell_x, cell_y):
    return cell_y * COUNT * COUNT + y * COUNT


def x_kernel(groups, density, ghost_below, ghost_above, weight, *refs):
    arrays, (out, rim_below, rim_above, swept, lower, upper, sends, receives, save), rest = refs[:7], refs[7:16], refs[16:]
    field, total, modes, mixed, *copies, loads = rest
    barrier, after, before = meet("gy")

    def prepare():
        neg = [density[c, :HALF, :] for c in range(2)] + [ghost_above[:HALF, :], ghost_above[HALF:, :]]
        nw = [weight[k, 0, :, :1] for k in range(3)]
        for c in range(2):
            swept[c, :HALF, :] = nw[0] * neg[c] + nw[1] * neg[c + 1] + nw[2] * neg[c + 2]
        pos = [ghost_below[:HALF, :], ghost_below[HALF:, :]] + [density[c, HALF:, :] for c in range(2)]
        pw = [weight[k, 1, :, :1] for k in range(3)]
        for c in range(2):
            new = pw[0] * pos[c + 2] + pw[1] * pos[c + 1] + pw[2] * pos[c]
            for row in range(HALF):
                swept[c, COUNT - 1 - row : COUNT - row, :] = new[row : row + 1]
        for half_y in range(2):
            for place in range(HALF):
                y = COUNT - 1 - place if half_y else place
                for g in range(groups):
                    parts = []
                    for s in range(CELLS):
                        at = piece(y, s // 2, 2 * g + s % 2)
                        parts.append(swept[s // 2, :, at : at + COUNT])
                    parts.append(jnp.zeros((COUNT, LANES - CELLS * COUNT), f32))
                    moved = jnp.concatenate(parts, 1)
                    rows = slice(place * HALF, (place + 1) * HALF)
                    field[half_y, rows, block(g)] = moved[:HALF]
                    field[2 + half_y, rows, block(g)] = moved[HALF:]

    collide(groups, field, total, modes, mixed, arrays, copies, loads, prepare)

    for q in range(4):
        field[q] = field[q] + collide_step * total[q]
    for half_x in range(2):
        pack(field, 2 * half_x, block(0), lower, half_x)
        pack(field, 2 * half_x + 1, block(groups - 1), upper, half_x)
    pl.semaphore_wait(barrier, 2)
    forth = passed(upper, rim_below, after, sends, receives, 0)
    back = passed(lower, rim_above, before, sends, receives, 1)
    forth.start()
    back.start()
    whole = pltpu.make_async_copy(field, out, save)
    whole.start()
    whole.wait()
    forth.wait()
    back.wait()


def pack(source, q, lanes, target, half_x):
    free = lax.broadcasted_iota(jnp.int32, (THIRD, LANES), 1) >= CELLS * COUNT
    rest = source[q, 3 * THIRD :, lanes]
    for k in range(3):
        kept = source[q, k * THIRD : (k + 1) * THIRD, lanes]
        start = (3 * half_x + k) * THIRD
        target[start : start + THIRD, :] = jnp.where(free, pltpu.roll(rest, CELLS * COUNT - k * SPARE, 1), kept)


def unpack(source, half_x, target):
    lane = lax.broadcasted_iota(jnp.int32, (THIRD, LANES), 1)
    rest = jnp.zeros((THIRD, LANES), f32)
    for k in range(3):
        start = (3 * half_x + k) * THIRD
        part = source[start : start + THIRD, :]
        target[k * THIRD : (k + 1) * THIRD, :] = jnp.where(lane < CELLS * COUNT, part, 0.0)
        rest = jnp.where(lane // SPARE == k, pltpu.roll(part, LANES - CELLS * COUNT + k * SPARE, 1), rest)
    target[3 * THIRD :, :] = rest


def y_kernel(groups, before, below, above, weight, *refs):
    arrays, (out, swept, rim, field, total, modes, mixed, *copies, loads) = refs[:7], refs[7:]

    def prepare():
        place = lax.broadcasted_iota(jnp.int32, (PLACES, LANES), 1) // COUNT
        odd = place % 2 == 1
        for half_x in range(2):
            for half_y in range(2):
                q = 2 * half_x + half_y
                w0, w1, w2 = [weight[k, half_y] for k in range(3)]
                blocks = [before[q, :, block(g)] for g in range(groups)]
                unpack(below if half_y else above, half_x, rim)
                blocks = [rim[...]] + blocks if half_y else blocks + [rim[...]]
                right = [pltpu.roll(b, COUNT, 1) for b in blocks]
                left = [pltpu.roll(b, LANES - COUNT, 1) for b in blocks]
                for g in range(groups):
                    if half_y:
                        near = jnp.where(odd, right[g + 1], left[g])
                        new = w0 * blocks[g + 1] + w1 * near + w2 * blocks[g]
                    else:
                        near = jnp.where(odd, right[g + 1], left[g])
                        new = w0 * blocks[g] + w1 * near + w2 * blocks[g + 1]
                    field[q, :, block(g)] = new

    collide(groups, field, total, modes, mixed, arrays, copies, loads, prepare)

    for q in range(4):
        field[q] = field[q] + collide_step * total[q]
    wide = 2 * COUNT * COUNT
    for g in range(groups):
        columns = []
        for y in range(COUNT):
            half_y, place = (0, y) if y < HALF else (1, COUNT - 1 - y)
            rows = slice(place * HALF, (place + 1) * HALF)
            columns.append(jnp.concatenate([field[half_y, rows, block(g)], field[2 + half_y, rows, block(g)]], 0))
        for c in range(2):
            parts = []
            for cell_y in range(2):
                at = (2 * c + cell_y) * COUNT
                parts += [column[:, at : at + COUNT] for column in columns]
            swept[c, :, g * wide : (g + 1) * wide] = jnp.concatenate(parts, 1)
    for c in range(2):
        out[c, :HALF, :] = swept[c, :HALF, :]
        for row in range(HALF):
            out[c, HALF + row : HALF + row + 1, :] = swept[c, COUNT - 1 - row : COUNT - row, :]


def call(kernel, groups, field_args, arrays, out_shapes, out_space, scratch, **settings):
    wide = groups * LANES
    inside = pl.BlockSpec(memory_space=pltpu.VMEM)
    terms = arrays[0].shape[0]
    return pl.pallas_call(
        functools.partial(kernel, groups),
        out_shape=out_shapes,
        in_specs=[inside] * len(field_args) + [pl.BlockSpec(memory_space=pl.ANY)] * len(arrays),
        out_specs=jax.tree.map(lambda _: pl.BlockSpec(memory_space=out_space), out_shapes),
        compiler_params=pltpu.CompilerParams(**settings),
        scratch_shapes=scratch
        + [pltpu.VMEM((4, PLACES, n * wide), f32) for n in (1, 1, 1, 2)]
        + [pltpu.VMEM(a.shape, a.dtype) for a in arrays]
        + [pltpu.SemaphoreType.DMA((3, max(terms, len(arrays))))],
    )(*field_args, *arrays)


def meet(axis):
    count = lax.axis_size(axis)
    me = lax.axis_index(axis)
    after, before = {axis: lax.rem(me + 1, count)}, {axis: lax.rem(me + count - 1, count)}
    barrier = pltpu.get_barrier_semaphore()
    for neighbour in (after, before):
        pl.semaphore_signal(barrier, inc=1, device_id=neighbour, device_id_type=pl.DeviceIdType.MESH)
    return barrier, after, before


def passed(source, target, device, sends, receives, index):
    return pltpu.make_async_remote_copy(
        src_ref=source,
        dst_ref=target,
        send_sem=sends.at[index],
        recv_sem=receives.at[index],
        device_id=device,
        device_id_type=pl.DeviceIdType.MESH,
    )


def spread(raw, wide, out):
    used = lax.broadcasted_iota(jnp.int32, (COUNT, LANES), 1) < COUNT
    for mode in range(COUNT):
        value = jnp.concatenate([raw[mode], jnp.zeros((COUNT, LANES - COUNT), f32)], 1)
        value = jnp.where(used, value, 0.0)
        value = value + pltpu.roll(value, COUNT, 1)
        wide[mode] = value + pltpu.roll(value, 2 * COUNT, 1)
    for parity_x in range(2):
        for parity_y in range(2):
            rows = [wide[2 * place + parity_x, pl.ds(parity_y, HALF, stride=2), :] for place in range(HALF)]
            for place in range(0, HALF, 2):
                out[2 * parity_x + parity_y, place * HALF : (place + 2) * HALF, :] = jnp.concatenate(rows[place : place + 2], 0)


def start_kernel(source, gain_a, gain_b, loss, below, above, out_a, out_b, out_loss, *refs):
    density, up, down, raw_a, raw_b, raw_loss, wide, made_a, made_b, made_loss, *sems = refs
    sends, receives, loads, saves, load_loss, save_loss, load_density = sems
    terms = raw_a.shape[0]
    barrier, after, before = meet("gx")
    whole = pltpu.make_async_copy(source, density, load_density)
    whole.start()
    sides = ((0, gain_a, raw_a, made_a, out_a), (1, gain_b, raw_b, made_b, out_b))

    def load(p, side):
        i, source, raw, _, _ = sides[side]
        return pltpu.make_async_copy(source.at[p], raw.at[p], loads.at[i, p])

    def save(p, side):
        i, _, _, made, out = sides[side]
        return pltpu.make_async_copy(made.at[p], out.at[p], saves.at[i, p])

    pltpu.make_async_copy(loss, raw_loss, load_loss).start()
    for side in range(2):
        lax.fori_loop(0, terms, lambda p, c: (load(p, side).start(), c)[1], 0)
    whole.wait()
    for c in range(2):
        up[c * HALF : (c + 1) * HALF, :] = density[c, HALF:, :]
        down[c * HALF : (c + 1) * HALF, :] = density[c, :HALF, :]
    pl.semaphore_wait(barrier, 2)
    forth = passed(up, below, after, sends, receives, 0)
    back = passed(down, above, before, sends, receives, 1)
    forth.start()
    back.start()
    pltpu.make_async_copy(loss, raw_loss, load_loss).wait()
    spread(raw_loss, wide, made_loss)
    pltpu.make_async_copy(made_loss, out_loss, save_loss).start()
    for side in range(2):

        def one(p, carry):
            load(p, side).wait()
            spread(sides[side][2].at[p], wide, sides[side][3].at[p])
            save(p, side).start()
            return carry

        lax.fori_loop(0, terms, one, 0)
    for side in range(2):
        lax.fori_loop(0, terms, lambda p, c: (save(p, side).wait(), c)[1], 0)
    pltpu.make_async_copy(made_loss, out_loss, save_loss).wait()
    forth.wait()
    back.wait()


def start(density, gains_a, gains_b, loss_rates):
    terms = gains_a.shape[0]
    rim = jax.ShapeDtypeStruct((COUNT, density.shape[2]), f32)
    gain = jax.ShapeDtypeStruct((terms, 4, PLACES, LANES), f32)
    loss = jax.ShapeDtypeStruct((4, PLACES, LANES), f32)
    anywhere = pl.BlockSpec(memory_space=pl.ANY)
    dma = pltpu.SemaphoreType.DMA
    return pl.pallas_call(
        start_kernel,
        out_shape=(rim, rim, gain, gain, loss),
        in_specs=[anywhere] * 4,
        out_specs=(anywhere,) * 5,
        scratch_shapes=[pltpu.VMEM(density.shape, f32)] + [pltpu.VMEM(rim.shape, f32)] * 2
        + [pltpu.VMEM(a.shape, f32) for a in (gains_a, gains_b, loss_rates)]
        + [pltpu.VMEM((COUNT + 1, COUNT, LANES), f32)]
        + [pltpu.VMEM(a.shape, f32) for a in (gain, gain, loss)]
        + [dma((2,)), dma((2,)), dma((2, terms)), dma((2, terms)), dma, dma, dma],
        compiler_params=pltpu.CompilerParams(collective_id=0, has_side_effects=True),
    )(density, gains_a, gains_b, loss_rates)


def body(density, gains_a, gains_b, loss_rates):
    count, merged = density.shape[1:]
    groups = merged // (2 * count * count)
    below, above, *gains = start(density, gains_a, gains_b, loss_rates)
    arrays = (*gains, *[jnp.asarray(t) for t in transform_tables()])
    inner = jax.ShapeDtypeStruct((4, PLACES, groups * LANES), f32)
    rim = jax.ShapeDtypeStruct((6 * THIRD, LANES), f32)
    swept = pltpu.VMEM((2, count, merged), f32)
    dma = pltpu.SemaphoreType.DMA
    rims = [pltpu.VMEM(rim.shape, f32)] * 2 + [dma((2,)), dma((2,)), dma]
    before = (density, below, above, jnp.asarray(x_weights()))
    settings = dict(collective_id=1, has_side_effects=True)
    field, below, above = call(x_kernel, groups, before, arrays, (inner, rim, rim), pl.ANY, [swept] + rims, **settings)
    out = jax.ShapeDtypeStruct(density.shape, f32)
    return call(y_kernel, groups, (field, below, above, jnp.asarray(y_weights())), arrays, out, pltpu.VMEM, [swept, pltpu.VMEM((PLACES, LANES), f32)])


def solution(mesh):
    in_specs = (P("gx", None, "gy"), P(), P(), P())
    out_specs = P("gx", None, "gy")
    return jax.shard_map(body, mesh=mesh, in_specs=in_specs, out_specs=out_specs, check_vma=False)
```
